32 devices in a mesh: tile: 16 (over z, y, core), shell: 2 (over x).
Axes of the slice: x: 2, y: 2, z: 4, core: 2. Of those that a mesh axis runs over, the one named last changes fastest.
Arguments:
- particles: bfloat16 [512, 2, 32768], P('tile', None, 'shell'), may hold values from -40 to 40
- projections: bfloat16 [512, 2, 32768], P('tile', None, 'shell'), may hold values from -6 to 6
- noise_weight: float32 [32768], P('shell'), may hold values from 0.001 to 0.012
- tile_list: int32 [512, 4], P('tile'), may hold values from 0 to 15, all different within a row; in each aligned block of 32 rows (0 to 31, 32 to 63, ...) at most 16 rows name the same one
- ori_start: int32 [512, 4], P('tile'), may hold values from 0 to 31
- shifts: int32 [512, 2], P('tile'), may hold values from -8 to 8
- defocus_bin: int32 [512], P('tile'), may hold values from 0 to 15
Outputs:
- posterior: float32 [512, 9, 64], P('tile')
- log_evidence: float32 [512], P('tile')
The draws below stay inside these ranges and needn't reach their ends.
Inputs may be any that keep to these rules, and one draw needn't show every extreme that they name: `tile_list`: the 4 tiles of one particle differ, and among the particles of one index of tile no tile is named more than 16 times, a count reached.
All inputs are finite; a program needn't handle non-finite values.
Results may differ from the reference program's by a relative error of at most 0.0035.
Values may be sent and summed in bfloat16 or wider, within the bound.
A program may use at most 192 MiB of HBM per device.

```python
import math
import jax
import jax.numpy as jnp
import numpy as np
from jax import lax

BOX = 256
K = 32768
ORI_DEV = 32
ORI_WIN = 16
N_ORI = 512
WIN = 4
P_DEV = 32
PARTICLES = 512
CAP = 16
NBIN = 16
TSIDE = 3
N_TILE = 16


def draw_particles(key, part):
    scale_key = jax.random.fold_in(key, 11)
    noise_key = jax.random.fold_in(key, 12)
    gauss = jax.random.normal(noise_key, (PARTICLES, 2, K), jnp.float32)
    scales = jnp.exp(jax.random.uniform(scale_key, (PARTICLES, 1, 1), jnp.float32, math.log(2.0), math.log(8.0)))
    values = scales * gauss
    return jnp.clip(values, -40.0, 40.0).astype(jnp.bfloat16)


def draw_projections(key, part):
    tile_key = jax.random.fold_in(key, 22)

    def one_tile(tile_index):
        block_key = jax.random.fold_in(tile_key, tile_index)
        raw = jax.random.normal(block_key, (ORI_DEV, 2, K), jnp.float32)
        spread = jnp.sqrt(jnp.mean(raw * raw, axis=(1, 2), keepdims=True))
        return jnp.clip(raw / spread, -6.0, 6.0).astype(jnp.bfloat16)
    tiles = lax.map(one_tile, jnp.arange(N_TILE, dtype=jnp.int32))
    return tiles.reshape(N_ORI, 2, K)


def touch_ends(drawn, rng, least, top_value):
    extent = drawn.shape
    place = [jax.random.randint(jax.random.fold_in(rng, axis), (), 0, extent[axis]) for axis in range(len(extent))]
    drawn = drawn.at[tuple(place)].set(least)
    longest = extent.index(max(extent))
    place[longest] = (place[longest] + 1) % extent[longest]
    return drawn.at[tuple(place)].set(top_value)


def block_levels(own_key, shape, pieces, least, top_value):
    factor_of, own = 1.0, jax.random.fold_in(own_key, 6)
    for axis_at, shards_of in pieces:
        steps = jnp.exp(jax.random.uniform(jax.random.fold_in(own, axis_at), (shards_of,), jnp.float32, least / len(pieces), top_value / len(pieces)))
        factor_of = factor_of * jnp.repeat(steps, shape[axis_at] // shards_of).reshape([-1 if axis == axis_at else 1 for axis in range(len(shape))])
    return factor_of


def routed_block(rng, own, number, rows, amount, top, most, slope):
    ranking = jax.random.permutation(rng, amount)
    crowded, ordinary = shares(amount, rows * top, most, slope, True), shares(amount, rows * top, most, slope, False)
    places = jnp.arange(amount)

    def named(lengths, turn):
        used = int((lengths > 0).sum())
        fixed = max(1, used // 4)
        passed = fixed + (places - fixed + turn * (used - fixed)) % max(1, amount - fixed)
        return jnp.zeros((amount,), jnp.int32).at[ranking[jnp.where(places < fixed, places, passed)]].set(jnp.asarray(lengths, jnp.int32))

    lengths = jnp.where(number % 4 == 0, named(crowded, number // 4), named(ordinary, number - number // 4 - 1))
    mixed = jax.random.permutation(jax.random.fold_in(own, 3), amount)
    giver, receiver = mixed[0:amount // 2 * 2:2], mixed[1:amount // 2 * 2:2]
    slack = jnp.minimum(lengths[giver] - 1, most - lengths[receiver]) // 2
    slack = jnp.where((giver == ranking[0]) | (receiver == ranking[0]) | (lengths[receiver] == 0), 0, jnp.maximum(slack, 0))
    passed = jax.random.randint(jax.random.fold_in(own, 4), (amount // 2,), 0, 1 << 20) % (slack + 1)
    lengths = lengths.at[giver].add(-passed).at[receiver].add(passed)
    items = jnp.searchsorted(jnp.cumsum(lengths), jnp.arange(rows * top), side="right").astype(jnp.int32)
    table = items.reshape(top, rows).T
    table = table[jax.random.permutation(jax.random.fold_in(own, 1), rows)]
    turn = jax.random.randint(jax.random.fold_in(own, 2), (rows, 1), 0, top)
    return jnp.take_along_axis(table, (jnp.arange(top)[None, :] + turn) % top, axis=1)


def shares(amount, total, most, lean, full):
    weights = [(1 << 20) // math.isqrt(grade ** lean) + 1 for grade in range(1, amount + 1)]
    largest = most if full else min(most, max(-(-total // amount), total * weights[0] // sum(weights)))
    least = 1 if total - largest >= amount - 1 else 0
    holding, surplus = [largest] + [least] * (amount - 1), total - largest - least * (amount - 1)
    while surplus > 0:
        free = [i for i in range(1, amount) if holding[i] < largest] or [i for i in range(1, amount) if holding[i] < most]
        pool, left = sum([weights[i] for i in free]), surplus
        for i in free:
            more = min(most - holding[i], max(1, left * weights[i] // pool), surplus)
            holding[i] = holding[i] + more
            surplus = surplus - more
    return np.array(holding)


def setup_inputs(seed: int = 0) -> dict:
    key_of = jax.random.split(jax.random.key(seed), 8)
    particles = draw_particles(jax.random.fold_in(key_of[7], 71), 0)
    projections = draw_projections(jax.random.fold_in(key_of[7], 71), 0)
    noise_weight = jnp.clip(jnp.exp(math.log(0.012) - 2.4849066 * jax.random.uniform(key_of[2], (K,), jnp.float32) ** block_levels(key_of[2], (K,), ((0, 2),), -0.2, 0.2)), 0.001, 0.012)
    tile_list_keys = jax.random.split(jax.random.fold_in(key_of[3], 1), PARTICLES // P_DEV)
    tile_list_turns = jax.random.permutation(jax.random.fold_in(key_of[3], 3), PARTICLES // P_DEV)
    tile_list = jax.vmap(lambda own, number: routed_block(jax.random.fold_in(key_of[3], 2), own, number, P_DEV, N_TILE, WIN, CAP, 2))(tile_list_keys, tile_list_turns).reshape((PARTICLES, WIN))
    ori_start = touch_ends(jax.random.randint(key_of[4], (PARTICLES, WIN), 0, ORI_DEV), jax.random.fold_in(key_of[4], 1), 0, ORI_DEV - 1).astype(jnp.int32)
    shifts = touch_ends(jax.random.randint(key_of[5], (PARTICLES, 2), -8, 9), jax.random.fold_in(key_of[5], 1), -8, 8).astype(jnp.int32)
    defocus_bin = touch_ends(jax.random.randint(key_of[6], (PARTICLES,), 0, NBIN), jax.random.fold_in(key_of[6], 1), 0, NBIN - 1).astype(jnp.int32)
    return {"particles": particles, "projections": projections, "noise_weight": noise_weight, "tile_list": tile_list, "ori_start": ori_start, "shifts": shifts, "defocus_bin": defocus_bin}


wave_length = 0.0197
aberration = 27000000.0
amplitude = 0.1
b_factor = 20.0
defocus_base = 5000.0
defocus_step = 500.0

def frequencies(first_index, span_count):
    flat_index = first_index + jnp.arange(span_count, dtype=jnp.int32)
    freq_x = flat_index // BOX
    freq_y = flat_index % BOX - BOX // 2
    return (freq_x, freq_y)

def ctf_table(freq_x, freq_y, bins_count):
    scaled_x = freq_x.astype(jnp.float32) / BOX
    scaled_y = freq_y.astype(jnp.float32) / BOX
    radius_sq = scaled_x * scaled_x + scaled_y * scaled_y
    defocus = defocus_base + defocus_step * jnp.arange(bins_count, dtype=jnp.float32)[:, None]
    aberr_phase = math.pi * wave_length * defocus * radius_sq[None, :] - 0.5 * math.pi * aberration * wave_length ** 3 * radius_sq[None, :] ** 2
    envelope = jnp.exp(-0.25 * b_factor * radius_sq)[None, :]
    return -(math.sqrt(1.0 - amplitude ** 2) * jnp.sin(aberr_phase) + amplitude * jnp.cos(aberr_phase)) * envelope

def rotation(freq_x, freq_y, mult_x, mult_y):
    phase_turns = jnp.mod(freq_x * mult_x + freq_y * mult_y, BOX)
    angles = phase_turns.astype(jnp.float32) * (2.0 * math.pi / BOX)
    return (jnp.cos(angles), jnp.sin(angles))

def pick_rows(bin_index, lookup):
    one_hot = (bin_index[:, None] == jnp.arange(lookup.shape[0], dtype=jnp.int32)[None, :]).astype(jnp.float32)
    return jnp.dot(one_hot, lookup, precision=lax.Precision.HIGHEST, preferred_element_type=jnp.float32)

def prepare(particles, weight, ctf_rows, shifts, freq_x, freq_y):
    values = particles.astype(jnp.float32)
    real_part = values[:, 0]
    imag_part = values[:, 1]
    cosine, sine_value = rotation(freq_x[None, :], freq_y[None, :], shifts[:, 0:1], shifts[:, 1:2])
    moved_real = real_part * cosine + imag_part * sine_value
    moved_imag = imag_part * cosine - real_part * sine_value
    factor = weight[None, :] * ctf_rows
    weighted = jnp.stack([factor * moved_real, factor * moved_imag], axis=1).astype(jnp.bfloat16)
    energy = lax.optimization_barrier(jnp.sum(weight[None, :] * (real_part * real_part + imag_part * imag_part), axis=1))
    return (weighted, energy)

def shifted_tables(projections, freq_x, freq_y):
    offsets = jnp.arange(TSIDE, dtype=jnp.int32) - TSIDE // 2
    mult_x = jnp.repeat(offsets, TSIDE)[:, None]
    mult_y = jnp.tile(offsets, TSIDE)[:, None]
    cosine, sine_value = rotation(freq_x[None, :], freq_y[None, :], mult_x, mult_y)
    cosine = cosine[:, None, :]
    sine_value = sine_value[:, None, :]
    proj_real = projections[:, 0].astype(jnp.float32)[None, :, :]
    proj_imag = projections[:, 1].astype(jnp.float32)[None, :, :]
    moved_real = proj_real * cosine - proj_imag * sine_value
    moved_imag = proj_imag * cosine + proj_real * sine_value
    stacked = jnp.stack([moved_real, moved_imag], axis=2).astype(jnp.bfloat16)
    return stacked.reshape(TSIDE * TSIDE * projections.shape[0], -1)

def slot_scores(slot_rows, bin_index, projections, weight, ctf, freq_x, freq_y):
    orient_count = projections.shape[0]
    lookup = shifted_tables(projections, freq_x, freq_y)
    cross_term = lax.dot_general(slot_rows, lookup, (((1,), (1,)), ((), ())), preferred_element_type=jnp.float32)
    cross_term = cross_term.reshape(slot_rows.shape[0], TSIDE * TSIDE, orient_count)
    proj_values = projections.astype(jnp.float32)
    magnitude = proj_values[:, 0] * proj_values[:, 0] + proj_values[:, 1] * proj_values[:, 1]
    weighted_ctf = weight[None, :] * ctf * ctf
    power = lax.dot_general(weighted_ctf, magnitude, (((1,), (1,)), ((), ())), precision=lax.Precision.HIGHEST, preferred_element_type=jnp.float32)
    power_rows = pick_rows(bin_index, power)
    return cross_term - 0.5 * power_rows[:, None, :]

def window(scores, starts, orient_count):
    orient_index = jnp.mod(starts[:, None] + jnp.arange(orient_count // 2, dtype=jnp.int32)[None, :], orient_count)
    return jnp.take_along_axis(scores, orient_index[:, None, :], axis=2)

def slot_layout(tile_ids, tile_count, capacity):
    positions = jnp.arange(tile_ids.shape[0], dtype=jnp.int32)
    earlier_same = (tile_ids[:, None] == tile_ids[None, :]) & (positions[None, :] < positions[:, None])
    slot_rank = lax.optimization_barrier(jnp.sum(earlier_same.astype(jnp.int32), axis=1))
    slot_index = tile_ids * capacity + slot_rank
    matches = slot_index[None, :] == jnp.arange(tile_count * capacity, dtype=jnp.int32)[:, None]
    slot_owner = lax.optimization_barrier(jnp.sum(jnp.where(matches, positions[None, :] + 1, 0), axis=1)) - 1
    return (slot_index, slot_owner)

def finish(scores, energy_sum):
    scored = scores - 0.5 * energy_sum[:, None, None]
    row_peak = lax.optimization_barrier(jnp.max(scored, axis=(1, 2)))
    log_total = row_peak + jnp.log(lax.optimization_barrier(jnp.sum(jnp.exp(scored - row_peak[:, None, None]), axis=(1, 2))))
    posterior = jnp.exp(scored - log_total[:, None, None])
    return (posterior, log_total)

def reference(particles, projections, noise_weight, tile_list, ori_start, shifts, defocus_bin):
    capacity = CAP
    freq_x, freq_y = frequencies(0, K)
    ctf = ctf_table(freq_x, freq_y, NBIN)

    def prep_block(block_index):
        first = block_index * P_DEV
        block_particles = lax.dynamic_slice_in_dim(particles, first, P_DEV, 0)
        block_shifts = lax.dynamic_slice_in_dim(shifts, first, P_DEV, 0)
        block_bins = lax.dynamic_slice_in_dim(defocus_bin, first, P_DEV, 0)
        return prepare(block_particles, noise_weight, pick_rows(block_bins, ctf), block_shifts, freq_x, freq_y)
    weighted, energy = lax.map(prep_block, jnp.arange(N_TILE, dtype=jnp.int32))
    weighted = weighted.reshape(PARTICLES, 2 * K)
    energy = energy.reshape(PARTICLES)
    block_tiles = tile_list.reshape(N_TILE, P_DEV * WIN)
    slots_all, owners_all = jax.vmap(lambda tile_ids: slot_layout(tile_ids, N_TILE, capacity))(block_tiles)
    starts_flat = ori_start.reshape(-1)

    def score_tile(tile_index):
        slot_owner = lax.dynamic_slice_in_dim(owners_all, tile_index * capacity, capacity, 1)
        source_index = jnp.arange(N_TILE, dtype=jnp.int32)[:, None]
        item_index = (source_index * (P_DEV * WIN) + jnp.maximum(slot_owner, 0)).reshape(-1)
        particle = item_index // WIN
        occupied = (slot_owner >= 0).reshape(-1)
        slot_rows = jnp.where(occupied[:, None], weighted[particle], jnp.zeros((), weighted.dtype))
        tile_proj = lax.dynamic_slice_in_dim(projections, tile_index * ORI_DEV, ORI_DEV, 0)
        partial_value = slot_scores(slot_rows, defocus_bin[particle], tile_proj, noise_weight, ctf, freq_x, freq_y)
        chosen = window(partial_value, starts_flat[item_index], ORI_DEV)
        return chosen.reshape(N_TILE, capacity, TSIDE * TSIDE, ORI_WIN)
    results = lax.map(score_tile, jnp.arange(N_TILE, dtype=jnp.int32))
    tiles_flat = tile_list.reshape(-1)
    source_of = jnp.arange(PARTICLES * WIN, dtype=jnp.int32) // (P_DEV * WIN)
    slot_rank = slots_all.reshape(-1) - tiles_flat * capacity
    returned = results[tiles_flat, source_of, slot_rank]
    returned = returned.reshape(PARTICLES, WIN, TSIDE * TSIDE, ORI_WIN)
    scores = jnp.transpose(returned, (0, 2, 1, 3)).reshape(PARTICLES, TSIDE * TSIDE, WIN * ORI_WIN)
    return finish(scores, energy)
```

```python
import functools
import math

import jax
import jax.numpy as jnp
from jax import lax
from jax.experimental import pallas as pl
from jax.experimental.pallas import tpu as pltpu
from jax.sharding import PartitionSpec as P

BOX = 256
NBIN = 16
TSIDE = 3


wave_length = 0.0197
aberration = 27000000.0
amplitude = 0.1
b_factor = 20.0
defocus_base = 5000.0
defocus_step = 500.0


def frequencies(first_index, span_count):
    flat_index = first_index + jnp.arange(span_count, dtype=jnp.int32)
    freq_x = flat_index // BOX
    freq_y = flat_index % BOX - BOX // 2
    return (freq_x, freq_y)


def ctf_table(freq_x, freq_y, bins_count):
    scaled_x = freq_x.astype(jnp.float32) / BOX
    scaled_y = freq_y.astype(jnp.float32) / BOX
    radius_sq = scaled_x * scaled_x + scaled_y * scaled_y
    defocus = defocus_base + defocus_step * jnp.arange(bins_count, dtype=jnp.float32)[:, None]
    aberr_phase = (
        math.pi * wave_length * defocus * radius_sq[None, :]
        - 0.5 * math.pi * aberration * wave_length**3 * radius_sq[None, :] ** 2
    )
    envelope = jnp.exp(-0.25 * b_factor * radius_sq)[None, :]
    return (
        -(math.sqrt(1.0 - amplitude**2) * jnp.sin(aberr_phase) + amplitude * jnp.cos(aberr_phase))
        * envelope
    )


def rotation(freq_x, freq_y, mult_x, mult_y):
    phase_turns = jnp.mod(freq_x * mult_x + freq_y * mult_y, BOX)
    angles = phase_turns.astype(jnp.float32) * (2.0 * math.pi / BOX)
    return (jnp.cos(angles), jnp.sin(angles))


def pick_rows(bin_index, lookup):
    one_hot = (bin_index[:, None] == jnp.arange(lookup.shape[0], dtype=jnp.int32)[None, :]).astype(
        jnp.float32
    )
    return jnp.dot(
        one_hot, lookup, precision=lax.Precision.HIGHEST, preferred_element_type=jnp.float32
    )


def prepare(particles, weight, ctf_rows, shifts, freq_x, freq_y):
    values = particles.astype(jnp.float32)
    real_part = values[:, 0]
    imag_part = values[:, 1]
    cosine, sine_value = rotation(freq_x[None, :], freq_y[None, :], shifts[:, 0:1], shifts[:, 1:2])
    moved_real = real_part * cosine + imag_part * sine_value
    moved_imag = imag_part * cosine - real_part * sine_value
    factor = weight[None, :] * ctf_rows
    weighted = jnp.stack([factor * moved_real, factor * moved_imag], axis=1).astype(jnp.bfloat16)
    energy = jnp.sum(weight[None, :] * (real_part * real_part + imag_part * imag_part), axis=1)
    return (weighted, energy)


def shifted_tables(projections, freq_x, freq_y):
    offsets = jnp.arange(TSIDE, dtype=jnp.int32) - TSIDE // 2
    mult_x = jnp.repeat(offsets, TSIDE)[:, None]
    mult_y = jnp.tile(offsets, TSIDE)[:, None]
    cosine, sine_value = rotation(freq_x[None, :], freq_y[None, :], mult_x, mult_y)
    cosine = cosine[:, None, :]
    sine_value = sine_value[:, None, :]
    proj_real = projections[:, 0].astype(jnp.float32)[None, :, :]
    proj_imag = projections[:, 1].astype(jnp.float32)[None, :, :]
    moved_real = proj_real * cosine - proj_imag * sine_value
    moved_imag = proj_imag * cosine + proj_real * sine_value
    stacked = jnp.stack([moved_real, moved_imag], axis=2).astype(jnp.bfloat16)
    return stacked.reshape(TSIDE * TSIDE * projections.shape[0], -1)


def slot_scores(slot_rows, bin_index, projections, weight, ctf, freq_x, freq_y):
    orient_count = projections.shape[0]
    lookup = shifted_tables(projections, freq_x, freq_y)
    cross_term = lax.dot_general(
        slot_rows, lookup, (((1,), (1,)), ((), ())), preferred_element_type=jnp.float32
    )
    cross_term = cross_term.reshape(slot_rows.shape[0], TSIDE * TSIDE, orient_count)
    proj_values = projections.astype(jnp.float32)
    magnitude = proj_values[:, 0] * proj_values[:, 0] + proj_values[:, 1] * proj_values[:, 1]
    weighted_ctf = weight[None, :] * ctf * ctf
    power = lax.dot_general(
        weighted_ctf,
        magnitude,
        (((1,), (1,)), ((), ())),
        precision=lax.Precision.HIGHEST,
        preferred_element_type=jnp.float32,
    )
    power_rows = pick_rows(bin_index, power)
    return cross_term - 0.5 * power_rows[:, None, :]


def window(scores, starts, orient_count):
    orient_index = jnp.mod(
        starts[:, None] + jnp.arange(orient_count // 2, dtype=jnp.int32)[None, :], orient_count
    )
    return jnp.take_along_axis(scores, orient_index[:, None, :], axis=2)


def slot_layout(tile_ids, tile_count, capacity):
    positions = jnp.arange(tile_ids.shape[0], dtype=jnp.int32)
    earlier_same = (tile_ids[:, None] == tile_ids[None, :]) & (
        positions[None, :] < positions[:, None]
    )
    slot_rank = jnp.sum(earlier_same.astype(jnp.int32), axis=1)
    slot_index = tile_ids * capacity + slot_rank
    matches = slot_index[None, :] == jnp.arange(tile_count * capacity, dtype=jnp.int32)[:, None]
    slot_owner = jnp.sum(jnp.where(matches, positions[None, :] + 1, 0), axis=1) - 1
    return (slot_index, slot_owner)


def finish(scores, energy_sum):
    scored = scores - 0.5 * energy_sum[:, None, None]
    row_peak = jnp.max(scored, axis=(1, 2))
    log_total = row_peak + jnp.log(jnp.sum(jnp.exp(scored - row_peak[:, None, None]), axis=(1, 2)))
    posterior = jnp.exp(scored - log_total[:, None, None])
    return (posterior, log_total)


def slot_plan(particles, projections, noise_weight, tile_list, ori_start, shifts, defocus_bin):
    tile_count = lax.axis_size("tile")
    band_index = lax.axis_index("shell")
    local_count = particles.shape[0]
    window_count = tile_list.shape[1]
    band_width = particles.shape[2]
    orient_count = projections.shape[0]
    capacity = max(2, (2 * local_count * window_count + tile_count - 1) // tile_count)
    freq_x, freq_y = frequencies(band_index * band_width, band_width)
    ctf = ctf_table(freq_x, freq_y, NBIN)
    weighted, energy = prepare(
        particles, noise_weight, pick_rows(defocus_bin, ctf), shifts, freq_x, freq_y
    )
    weighted = weighted.reshape(local_count, 2 * band_width)
    slot_index, slot_owner = slot_layout(tile_list.reshape(-1), tile_count, capacity)
    occupied = slot_owner >= 0
    item_index = jnp.maximum(slot_owner, 0)
    particle = item_index // window_count
    starts_flat = ori_start.reshape(-1)
    send_rows = jnp.where(
        occupied[:, None], jnp.take(weighted, particle, axis=0), jnp.zeros((), jnp.bfloat16)
    )
    send_rows = send_rows.reshape(tile_count, capacity, 2 * band_width)
    send_labels = jnp.stack(
        [jnp.take(defocus_bin, particle), jnp.take(starts_flat, item_index)], axis=1
    )
    send_labels = send_labels.astype(jnp.bfloat16).reshape(tile_count, capacity, 2)
    payload = lax.all_to_all(send_rows, "tile", split_axis=0, concat_axis=0, tiled=True)
    labels = lax.all_to_all(send_labels, "tile", split_axis=0, concat_axis=0, tiled=True)
    source_count = payload.shape[0]
    slot_count = payload.shape[1]
    slot_rows = payload.reshape(source_count * slot_count, payload.shape[2])
    label_ints = labels.reshape(source_count * slot_count, 2).astype(jnp.int32)
    partial_value = slot_scores(
        slot_rows, label_ints[:, 0], projections, noise_weight, ctf, freq_x, freq_y
    )
    partial_value = partial_value.reshape(
        source_count, slot_count, partial_value.shape[1], partial_value.shape[2]
    )
    returned = lax.all_to_all(partial_value, "tile", split_axis=0, concat_axis=0, tiled=True)
    candidates = returned.shape[2]
    returned = jnp.take(
        returned.reshape(tile_count * capacity, candidates, returned.shape[3]), slot_index, axis=0
    )
    returned = window(returned, starts_flat, orient_count)
    kept = returned.shape[2]
    returned = returned.reshape(local_count, window_count, candidates, kept)
    scores = jnp.transpose(returned, (0, 2, 1, 3)).reshape(
        local_count, candidates, window_count * kept
    )
    scores, energy_sum = lax.psum((scores, energy), "shell")
    return finish(scores, energy_sum)


SHIFT_MAX = 8
HIGH = lax.Precision.HIGHEST


def round_up(value, step):
    return (value + step - 1) // step * step


def weigh_kernel(part_ref, factor_ref, wave_y_ref, wave_x_ref, weight_ref, out_ref, energy_ref):
    rows, width = factor_ref.shape
    lines = width // BOX
    energy = jnp.zeros((rows, 1), jnp.float32)
    cos_y = wave_y_ref[:, :BOX]
    sin_y = wave_y_ref[:, BOX:]
    for line in range(lines):
        span = pl.ds(line * BOX, BOX)
        real_part = part_ref[0, 0, :, span].astype(jnp.float32)
        imag_part = part_ref[0, 1, :, span].astype(jnp.float32)
        cos_x = wave_x_ref[:, line : line + 1]
        sin_x = wave_x_ref[:, lines + line : lines + line + 1]
        cosine = cos_x * cos_y - sin_x * sin_y
        sine_value = sin_x * cos_y + cos_x * sin_y
        factor = factor_ref[:, span]
        out_ref[:, span] = (factor * (real_part * cosine + imag_part * sine_value)).astype(
            jnp.bfloat16
        )
        out_ref[:, pl.ds(width + line * BOX, BOX)] = (
            factor * (imag_part * cosine - real_part * sine_value)
        ).astype(jnp.bfloat16)
        square = real_part * real_part + imag_part * imag_part
        energy += jnp.sum(weight_ref[:, span] * square, axis=1, keepdims=True)
    energy_ref[...] = energy


def score_kernel(
    orients,
    proj_ref,
    power_ref,
    weighted_ref,
    energy_ref,
    hot_ref,
    tiles_ref,
    starts_ref,
    cos_ref,
    sin_ref,
    out_ref,
    moved_ref,
    chosen_ref,
    final_ref,
):
    step = pl.program_id(0)
    tiles = proj_ref.shape[0]
    width = proj_ref.shape[3]
    cands = TSIDE * TSIDE
    windows = tiles_ref.shape[0]
    block = cands * orients
    middle = cands // 2
    for tile in range(tiles):
        real_part = proj_ref[tile, 0].astype(jnp.float32)
        imag_part = proj_ref[tile, 1].astype(jnp.float32)

        def put(cand, real_value, imag_value):
            rows = pl.ds(tile * block + cand * orients, orients)
            moved_ref[rows, :width] = real_value.astype(jnp.bfloat16)
            moved_ref[rows, width:] = imag_value.astype(jnp.bfloat16)

        put(middle, real_part, imag_part)
        for cand in range(middle):
            cosine = cos_ref[cand : cand + 1, :]
            sine_value = sin_ref[cand : cand + 1, :]
            real_cos = real_part * cosine
            imag_sin = imag_part * sine_value
            imag_cos = imag_part * cosine
            real_sin = real_part * sine_value
            put(cand, real_cos - imag_sin, imag_cos + real_sin)
            put(cands - 1 - cand, real_cos + imag_sin, imag_cos - real_sin)
    cross = lax.dot_general(
        moved_ref[...],
        weighted_ref[...],
        (((1,), (1,)), ((), ())),
        preferred_element_type=jnp.float32,
    )
    power = jnp.dot(
        power_ref[...], hot_ref[...], precision=HIGH, preferred_element_type=jnp.float32
    )
    for tile in range(tiles):
        half_power = 0.5 * power[tile * orients : (tile + 1) * orients]
        named = [tiles_ref[j : j + 1, :] == step * tiles + tile for j in range(windows)]
        for cand in range(cands):
            first = tile * block + cand * orients
            value = cross[first : first + orients] - half_power
            rows = pl.ds(cand * orients, orients)
            for j in range(windows):
                chosen_ref[j, rows, :] = jnp.where(named[j], value, chosen_ref[j, rows, :])

    @pl.when(step == pl.num_programs(0) - 1)
    def _():
        kept = orients // 2
        used = cands * windows * kept
        for j in range(windows):
            start = starts_ref[j : j + 1, :]
            for cand in range(cands):
                value = chosen_ref[j, pl.ds(cand * orients, orients), :]
                bit = orients // 2
                while bit:
                    turned = pltpu.roll(value, orients - bit, 0)
                    value = jnp.where((start & bit) != 0, turned, value)
                    bit //= 2
                final_ref[pl.ds((cand * windows + j) * kept, kept), :] = value[:kept]
        spare = final_ref.shape[0] - used
        final_ref[pl.ds(used, spare), :] = jnp.zeros((spare, final_ref.shape[1]), jnp.float32)
        turned = final_ref[...].T
        column = lax.broadcasted_iota(jnp.int32, turned.shape, 1)
        out_ref[...] = jnp.where(column >= used, energy_ref[...], turned)


def exchange(values, tile_count):
    rows, pair, band_width = values.shape
    blocks = values.reshape(rows, pair, tile_count, band_width // tile_count)
    blocks = jnp.transpose(blocks, (2, 1, 0, 3))
    return lax.all_to_all(blocks, "tile", split_axis=0, concat_axis=0, tiled=True)


def band_plan(particles, projections, noise_weight, tile_list, ori_start, shifts, defocus_bin):
    tile_count = lax.axis_size("tile")
    tile_index = lax.axis_index("tile")
    band_index = lax.axis_index("shell")
    local_count, pair, band_width = particles.shape
    orients = projections.shape[0]
    windows = tile_list.shape[1]
    width = band_width // tile_count
    lines = width // BOX
    count = local_count * tile_count
    cands = TSIDE * TSIDE

    labels = jnp.concatenate([tile_list, ori_start, shifts, defocus_bin[:, None]], axis=1).T
    labels = lax.all_gather(labels, "tile", axis=1, tiled=True)
    part_in = exchange(particles, tile_count)
    proj_in = exchange(projections, tile_count)

    tiles_all = labels[:windows]
    starts_all = labels[windows : 2 * windows]
    shift_x = labels[2 * windows]
    shift_y = labels[2 * windows + 1]
    bins = labels[2 * windows + 2]

    freq_x, freq_y = frequencies(band_index * band_width + tile_index * width, width)
    weight = lax.dynamic_slice_in_dim(noise_weight, tile_index * width, width, 0)
    ctf = ctf_table(freq_x, freq_y, NBIN)
    factor = pick_rows(bins, weight[None, :] * ctf)
    steps = jnp.arange(2 * SHIFT_MAX + 1, dtype=jnp.int32) - SHIFT_MAX
    none = jnp.zeros((), jnp.int32)
    own_y = jnp.arange(BOX, dtype=jnp.int32) - BOX // 2
    own_x = freq_x[::BOX]
    table_y = jnp.concatenate(rotation(own_y[None, :], own_y[None, :], none, steps[:, None]), axis=1)
    table_x = jnp.concatenate(rotation(own_x[None, :], own_x[None, :], steps[:, None], none), axis=1)
    wave_y = pick_rows(shift_y + SHIFT_MAX, table_y)
    wave_x = pick_rows(shift_x + SHIFT_MAX, table_x)

    weighted, energy = pl.pallas_call(
        weigh_kernel,
        grid=(tile_count,),
        in_specs=[
            pl.BlockSpec((1, pair, local_count, width), lambda i: (i, 0, 0, 0)),
            pl.BlockSpec((local_count, width), lambda i: (i, 0)),
            pl.BlockSpec((local_count, 2 * BOX), lambda i: (i, 0)),
            pl.BlockSpec((local_count, 2 * lines), lambda i: (i, 0)),
            pl.BlockSpec((1, width), lambda i: (0, 0)),
        ],
        out_specs=[
            pl.BlockSpec((local_count, pair * width), lambda i: (i, 0)),
            pl.BlockSpec((local_count, 1), lambda i: (i, 0)),
        ],
        out_shape=[
            jax.ShapeDtypeStruct((count, pair * width), jnp.bfloat16),
            jax.ShapeDtypeStruct((count, 1), jnp.float32),
        ],
        name="weigh",
    )(part_in, factor, wave_y, wave_x, weight[None, :])

    values = proj_in.astype(jnp.float32)
    magnitude = values[:, 0] * values[:, 0] + values[:, 1] * values[:, 1]
    power = lax.dot_general(
        magnitude.reshape(tile_count * orients, width),
        weight[None, :] * ctf * ctf,
        (((1,), (1,)), ((), ())),
        precision=HIGH,
        preferred_element_type=jnp.float32,
    )
    hot = (jnp.arange(NBIN, dtype=jnp.int32)[:, None] == bins[None, :]).astype(jnp.float32)
    offsets = jnp.arange(TSIDE, dtype=jnp.int32) - TSIDE // 2
    cos_t, sin_t = rotation(
        freq_x[None, :],
        freq_y[None, :],
        jnp.repeat(offsets, TSIDE)[:, None],
        jnp.tile(offsets, TSIDE)[:, None],
    )
    group = 2 if tile_count % 2 == 0 else 1
    used = cands * windows * (orients // 2)
    columns = round_up(used + 1, 128)

    def whole(*shape):
        return pl.BlockSpec(shape, lambda i: (0,) * len(shape))

    partial_value = pl.pallas_call(
        functools.partial(score_kernel, orients),
        grid=(tile_count // group,),
        in_specs=[
            pl.BlockSpec((group, pair, orients, width), lambda i: (i, 0, 0, 0)),
            pl.BlockSpec((group * orients, NBIN), lambda i: (i, 0)),
            whole(count, pair * width),
            whole(count, 1),
            whole(NBIN, count),
            whole(windows, count),
            whole(windows, count),
            whole(cands, width),
            whole(cands, width),
        ],
        out_specs=whole(count, columns),
        out_shape=jax.ShapeDtypeStruct((count, columns), jnp.float32),
        scratch_shapes=[
            pltpu.VMEM((group * cands * orients, pair * width), jnp.bfloat16),
            pltpu.VMEM((windows, cands * orients, count), jnp.float32),
            pltpu.VMEM((columns, count), jnp.float32),
        ],
        compiler_params=pltpu.CompilerParams(vmem_limit_bytes=48 * 1024 * 1024),
        name="score",
    )(proj_in, power, weighted, energy, hot, tiles_all, starts_all, cos_t, sin_t)

    blocks = partial_value.reshape(tile_count, local_count, columns)
    blocks = lax.all_to_all(blocks, "tile", split_axis=0, concat_axis=0, tiled=True)
    summed = jnp.sum(blocks, axis=0)
    summed = jnp.sum(lax.all_gather(summed, "shell", axis=0), axis=0)
    scores = summed[:, :used].reshape(local_count, cands, windows * (orients // 2))
    return finish(scores, summed[:, used])


def per_device(particles, projections, noise_weight, tile_list, ori_start, shifts, defocus_bin):
    piece = BOX * lax.axis_size("tile")
    plan = band_plan if particles.shape[2] % piece == 0 else slot_plan
    return plan(
        particles, projections, noise_weight, tile_list, ori_start, shifts, defocus_bin
    )


def solution(mesh):
    in_specs = (
        P("tile", None, "shell"),
        P("tile", None, "shell"),
        P("shell"),
        P("tile", None),
        P("tile", None),
        P("tile", None),
        P("tile"),
    )
    out_specs = (P("tile", None, None), P("tile"))
    return jax.shard_map(
        per_device, mesh=mesh, in_specs=in_specs, out_specs=out_specs, check_vma=False
    )
```

```python
import functools
import math

import jax
import jax.numpy as jnp
from jax import lax
from jax.experimental import pallas as pl
from jax.experimental.pallas import tpu as pltpu
from jax.sharding import PartitionSpec as P

BOX = 256
NBIN = 16
TSIDE = 3


wave_length = 0.0197
aberration = 27000000.0
amplitude = 0.1
b_factor = 20.0
defocus_base = 5000.0
defocus_step = 500.0


def frequencies(first_index, span_count):
    flat_index = first_index + jnp.arange(span_count, dtype=jnp.int32)
    freq_x = flat_index // BOX
    freq_y = flat_index % BOX - BOX // 2
    return (freq_x, freq_y)


def ctf_table(freq_x, freq_y, bins_count):
    scaled_x = freq_x.astype(jnp.float32) / BOX
    scaled_y = freq_y.astype(jnp.float32) / BOX
    radius_sq = scaled_x * scaled_x + scaled_y * scaled_y
    defocus = defocus_base + defocus_step * jnp.arange(bins_count, dtype=jnp.float32)[:, None]
    aberr_phase = (
        math.pi * wave_length * defocus * radius_sq[None, :]
        - 0.5 * math.pi * aberration * wave_length**3 * radius_sq[None, :] ** 2
    )
    envelope = jnp.exp(-0.25 * b_factor * radius_sq)[None, :]
    return (
        -(math.sqrt(1.0 - amplitude**2) * jnp.sin(aberr_phase) + amplitude * jnp.cos(aberr_phase))
        * envelope
    )


def rotation(freq_x, freq_y, mult_x, mult_y):
    phase_turns = jnp.mod(freq_x * mult_x + freq_y * mult_y, BOX)
    angles = phase_turns.astype(jnp.float32) * (2.0 * math.pi / BOX)
    return (jnp.cos(angles), jnp.sin(angles))


def pick_rows(bin_index, lookup):
    one_hot = (bin_index[:, None] == jnp.arange(lookup.shape[0], dtype=jnp.int32)[None, :]).astype(
        jnp.float32
    )
    return jnp.dot(
        one_hot, lookup, precision=lax.Precision.HIGHEST, preferred_element_type=jnp.float32
    )


def prepare(particles, weight, ctf_rows, shifts, freq_x, freq_y):
    values = particles.astype(jnp.float32)
    real_part = values[:, 0]
    imag_part = values[:, 1]
    cosine, sine_value = rotation(freq_x[None, :], freq_y[None, :], shifts[:, 0:1], shifts[:, 1:2])
    moved_real = real_part * cosine + imag_part * sine_value
    moved_imag = imag_part * cosine - real_part * sine_value
    factor = weight[None, :] * ctf_rows
    weighted = jnp.stack([factor * moved_real, factor * moved_imag], axis=1).astype(jnp.bfloat16)
    energy = jnp.sum(weight[None, :] * (real_part * real_part + imag_part * imag_part), axis=1)
    return (weighted, energy)


def shifted_tables(projections, freq_x, freq_y):
    offsets = jnp.arange(TSIDE, dtype=jnp.int32) - TSIDE // 2
    mult_x = jnp.repeat(offsets, TSIDE)[:, None]
    mult_y = jnp.tile(offsets, TSIDE)[:, None]
    cosine, sine_value = rotation(freq_x[None, :], freq_y[None, :], mult_x, mult_y)
    cosine = cosine[:, None, :]
    sine_value = sine_value[:, None, :]
    proj_real = projections[:, 0].astype(jnp.float32)[None, :, :]
    proj_imag = projections[:, 1].astype(jnp.float32)[None, :, :]
    moved_real = proj_real * cosine - proj_imag * sine_value
    moved_imag = proj_imag * cosine + proj_real * sine_value
    stacked = jnp.stack([moved_real, moved_imag], axis=2).astype(jnp.bfloat16)
    return stacked.reshape(TSIDE * TSIDE * projections.shape[0], -1)


def slot_scores(slot_rows, bin_index, projections, weight, ctf, freq_x, freq_y):
    orient_count = projections.shape[0]
    lookup = shifted_tables(projections, freq_x, freq_y)
    cross_term = lax.dot_general(
        slot_rows, lookup, (((1,), (1,)), ((), ())), preferred_element_type=jnp.float32
    )
    cross_term = cross_term.reshape(slot_rows.shape[0], TSIDE * TSIDE, orient_count)
    proj_values = projections.astype(jnp.float32)
    magnitude = proj_values[:, 0] * proj_values[:, 0] + proj_values[:, 1] * proj_values[:, 1]
    weighted_ctf = weight[None, :] * ctf * ctf
    power = lax.dot_general(
        weighted_ctf,
        magnitude,
        (((1,), (1,)), ((), ())),
        precision=lax.Precision.HIGHEST,
        preferred_element_type=jnp.float32,
    )
    power_rows = pick_rows(bin_index, power)
    return cross_term - 0.5 * power_rows[:, None, :]


def window(scores, starts, orient_count):
    orient_index = jnp.mod(
        starts[:, None] + jnp.arange(orient_count // 2, dtype=jnp.int32)[None, :], orient_count
    )
    return jnp.take_along_axis(scores, orient_index[:, None, :], axis=2)


def slot_layout(tile_ids, tile_count, capacity):
    positions = jnp.arange(tile_ids.shape[0], dtype=jnp.int32)
    earlier_same = (tile_ids[:, None] == tile_ids[None, :]) & (
        positions[None, :] < positions[:, None]
    )
    slot_rank = jnp.sum(earlier_same.astype(jnp.int32), axis=1)
    slot_index = tile_ids * capacity + slot_rank
    matches = slot_index[None, :] == jnp.arange(tile_count * capacity, dtype=jnp.int32)[:, None]
    slot_owner = jnp.sum(jnp.where(matches, positions[None, :] + 1, 0), axis=1) - 1
    return (slot_index, slot_owner)


def finish(scores, energy_sum):
    scored = scores - 0.5 * energy_sum[:, None, None]
    row_peak = jnp.max(scored, axis=(1, 2))
    log_total = row_peak + jnp.log(jnp.sum(jnp.exp(scored - row_peak[:, None, None]), axis=(1, 2)))
    posterior = jnp.exp(scored - log_total[:, None, None])
    return (posterior, log_total)


def slot_plan(particles, projections, noise_weight, tile_list, ori_start, shifts, defocus_bin):
    tile_count = lax.axis_size("tile")
    band_index = lax.axis_index("shell")
    local_count = particles.shape[0]
    window_count = tile_list.shape[1]
    band_width = particles.shape[2]
    orient_count = projections.shape[0]
    capacity = max(2, (2 * local_count * window_count + tile_count - 1) // tile_count)
    freq_x, freq_y = frequencies(band_index * band_width, band_width)
    ctf = ctf_table(freq_x, freq_y, NBIN)
    weighted, energy = prepare(
        particles, noise_weight, pick_rows(defocus_bin, ctf), shifts, freq_x, freq_y
    )
    weighted = weighted.reshape(local_count, 2 * band_width)
    slot_index, slot_owner = slot_layout(tile_list.reshape(-1), tile_count, capacity)
    occupied = slot_owner >= 0
    item_index = jnp.maximum(slot_owner, 0)
    particle = item_index // window_count
    starts_flat = ori_start.reshape(-1)
    send_rows = jnp.where(
        occupied[:, None], jnp.take(weighted, particle, axis=0), jnp.zeros((), jnp.bfloat16)
    )
    send_rows = send_rows.reshape(tile_count, capacity, 2 * band_width)
    send_labels = jnp.stack(
        [jnp.take(defocus_bin, particle), jnp.take(starts_flat, item_index)], axis=1
    )
    send_labels = send_labels.astype(jnp.bfloat16).reshape(tile_count, capacity, 2)
    payload = lax.all_to_all(send_rows, "tile", split_axis=0, concat_axis=0, tiled=True)
    labels = lax.all_to_all(send_labels, "tile", split_axis=0, concat_axis=0, tiled=True)
    source_count = payload.shape[0]
    slot_count = payload.shape[1]
    slot_rows = payload.reshape(source_count * slot_count, payload.shape[2])
    label_ints = labels.reshape(source_count * slot_count, 2).astype(jnp.int32)
    partial_value = slot_scores(
        slot_rows, label_ints[:, 0], projections, noise_weight, ctf, freq_x, freq_y
    )
    partial_value = partial_value.reshape(
        source_count, slot_count, partial_value.shape[1], partial_value.shape[2]
    )
    returned = lax.all_to_all(partial_value, "tile", split_axis=0, concat_axis=0, tiled=True)
    candidates = returned.shape[2]
    returned = jnp.take(
        returned.reshape(tile_count * capacity, candidates, returned.shape[3]), slot_index, axis=0
    )
    returned = window(returned, starts_flat, orient_count)
    kept = returned.shape[2]
    returned = returned.reshape(local_count, window_count, candidates, kept)
    scores = jnp.transpose(returned, (0, 2, 1, 3)).reshape(
        local_count, candidates, window_count * kept
    )
    scores, energy_sum = lax.psum((scores, energy), "shell")
    return finish(scores, energy_sum)


SHIFT_MAX = 8
HIGH = lax.Precision.HIGHEST


def round_up(value, step):
    return (value + step - 1) // step * step


def weigh_kernel(part_ref, factor_ref, wave_y_ref, wave_x_ref, weight_ref, out_ref, energy_ref):
    rows, width = factor_ref.shape
    lines = width // BOX
    energy = jnp.zeros((rows, 1), jnp.float32)
    cos_y = wave_y_ref[:, :BOX]
    sin_y = wave_y_ref[:, BOX:]
    for line in range(lines):
        span = pl.ds(line * BOX, BOX)
        real_part = part_ref[0, 0, :, span].astype(jnp.float32)
        imag_part = part_ref[0, 1, :, span].astype(jnp.float32)
        cos_x = wave_x_ref[:, line : line + 1]
        sin_x = wave_x_ref[:, lines + line : lines + line + 1]
        cosine = cos_x * cos_y - sin_x * sin_y
        sine_value = sin_x * cos_y + cos_x * sin_y
        factor = factor_ref[:, span]
        out_ref[:, span] = (factor * (real_part * cosine + imag_part * sine_value)).astype(
            jnp.bfloat16
        )
        out_ref[:, pl.ds(width + line * BOX, BOX)] = (
            factor * (imag_part * cosine - real_part * sine_value)
        ).astype(jnp.bfloat16)
        square = real_part * real_part + imag_part * imag_part
        energy += jnp.sum(weight_ref[:, span] * square, axis=1, keepdims=True)
    energy_ref[...] = energy


def score_kernel(
    orients,
    proj_ref,
    power_ref,
    weighted_ref,
    energy_ref,
    hot_ref,
    tiles_ref,
    starts_ref,
    cos_ref,
    sin_ref,
    out_ref,
    moved_ref,
    chosen_ref,
    final_ref,
):
    step = pl.program_id(0)
    tiles = proj_ref.shape[0]
    width = proj_ref.shape[3]
    cands = TSIDE * TSIDE
    windows = tiles_ref.shape[0]
    block = cands * orients
    middle = cands // 2
    for tile in range(tiles):
        real_part = proj_ref[tile, 0].astype(jnp.float32)
        imag_part = proj_ref[tile, 1].astype(jnp.float32)

        def put(cand, real_value, imag_value):
            rows = pl.ds(tile * block + cand * orients, orients)
            moved_ref[rows, :width] = real_value.astype(jnp.bfloat16)
            moved_ref[rows, width:] = imag_value.astype(jnp.bfloat16)

        put(middle, real_part, imag_part)
        for cand in range(middle):
            cosine = cos_ref[cand : cand + 1, :]
            sine_value = sin_ref[cand : cand + 1, :]
            real_cos = real_part * cosine
            imag_sin = imag_part * sine_value
            imag_cos = imag_part * cosine
            real_sin = real_part * sine_value
            put(cand, real_cos - imag_sin, imag_cos + real_sin)
            put(cands - 1 - cand, real_cos + imag_sin, imag_cos - real_sin)
    cross = lax.dot_general(
        moved_ref[...],
        weighted_ref[...],
        (((1,), (1,)), ((), ())),
        preferred_element_type=jnp.float32,
    )
    power = jnp.dot(
        power_ref[...], hot_ref[...], precision=HIGH, preferred_element_type=jnp.float32
    )
    for tile in range(tiles):
        half_power = 0.5 * power[tile * orients : (tile + 1) * orients]
        named = [tiles_ref[j : j + 1, :] == step * tiles + tile for j in range(windows)]
        for cand in range(cands):
            first = tile * block + cand * orients
            value = cross[first : first + orients] - half_power
            rows = pl.ds(cand * orients, orients)
            for j in range(windows):
                chosen_ref[j, rows, :] = jnp.where(named[j], value, chosen_ref[j, rows, :])

    @pl.when(step == pl.num_programs(0) - 1)
    def _():
        kept = orients // 2
        used = cands * windows * kept
        for j in range(windows):
            start = starts_ref[j : j + 1, :]
            for cand in range(cands):
                value = chosen_ref[j, pl.ds(cand * orients, orients), :]
                bit = orients // 2
                while bit:
                    turned = pltpu.roll(value, orients - bit, 0)
                    value = jnp.where((start & bit) != 0, turned, value)
                    bit //= 2
                final_ref[pl.ds((cand * windows + j) * kept, kept), :] = value[:kept]
        spare = final_ref.shape[0] - used
        final_ref[pl.ds(used, spare), :] = jnp.zeros((spare, final_ref.shape[1]), jnp.float32)
        turned = final_ref[...].T
        column = lax.broadcasted_iota(jnp.int32, turned.shape, 1)
        out_ref[...] = jnp.where(column >= used, energy_ref[...], turned)


def split_band(values, tile_count):
    rows, pair, band_width = values.shape
    blocks = values.reshape(rows, pair, tile_count, band_width // tile_count)
    return jnp.transpose(blocks, (2, 1, 0, 3))


def exchange(blocks):
    return lax.all_to_all(blocks, "tile", split_axis=0, concat_axis=0, tiled=True)


def band_plan(particles, projections, noise_weight, tile_list, ori_start, shifts, defocus_bin):
    tile_count = lax.axis_size("tile")
    tile_index = lax.axis_index("tile")
    band_index = lax.axis_index("shell")
    local_count, pair, band_width = particles.shape
    orients = projections.shape[0]
    windows = tile_list.shape[1]
    width = band_width // tile_count
    lines = width // BOX
    count = local_count * tile_count
    cands = TSIDE * TSIDE

    labels = jnp.concatenate([tile_list, ori_start, shifts, defocus_bin[:, None]], axis=1).T
    labels = lax.all_gather(labels, "tile", axis=1, tiled=True)
    part_blocks, labels = lax.optimization_barrier((split_band(particles, tile_count), labels))
    part_in = exchange(part_blocks)
    proj_blocks, part_in = lax.optimization_barrier((split_band(projections, tile_count), part_in))
    proj_in = exchange(proj_blocks)

    tiles_all = labels[:windows]
    starts_all = labels[windows : 2 * windows]
    shift_x = labels[2 * windows]
    shift_y = labels[2 * windows + 1]
    bins = labels[2 * windows + 2]

    freq_x, freq_y = frequencies(band_index * band_width + tile_index * width, width)
    weight = lax.dynamic_slice_in_dim(noise_weight, tile_index * width, width, 0)
    ctf = ctf_table(freq_x, freq_y, NBIN)
    factor = pick_rows(bins, weight[None, :] * ctf)
    steps = jnp.arange(2 * SHIFT_MAX + 1, dtype=jnp.int32) - SHIFT_MAX
    none = jnp.zeros((), jnp.int32)
    own_y = jnp.arange(BOX, dtype=jnp.int32) - BOX // 2
    own_x = freq_x[::BOX]
    table_y = jnp.concatenate(rotation(own_y[None, :], own_y[None, :], none, steps[:, None]), axis=1)
    table_x = jnp.concatenate(rotation(own_x[None, :], own_x[None, :], steps[:, None], none), axis=1)
    wave_y = pick_rows(shift_y + SHIFT_MAX, table_y)
    wave_x = pick_rows(shift_x + SHIFT_MAX, table_x)

    weighted, energy = pl.pallas_call(
        weigh_kernel,
        grid=(tile_count,),
        in_specs=[
            pl.BlockSpec((1, pair, local_count, width), lambda i: (i, 0, 0, 0)),
            pl.BlockSpec((local_count, width), lambda i: (i, 0)),
            pl.BlockSpec((local_count, 2 * BOX), lambda i: (i, 0)),
            pl.BlockSpec((local_count, 2 * lines), lambda i: (i, 0)),
            pl.BlockSpec((1, width), lambda i: (0, 0)),
        ],
        out_specs=[
            pl.BlockSpec((local_count, pair * width), lambda i: (i, 0)),
            pl.BlockSpec((local_count, 1), lambda i: (i, 0)),
        ],
        out_shape=[
            jax.ShapeDtypeStruct((count, pair * width), jnp.bfloat16),
            jax.ShapeDtypeStruct((count, 1), jnp.float32),
        ],
        name="weigh",
    )(part_in, factor, wave_y, wave_x, weight[None, :])

    values = proj_in.astype(jnp.float32)
    magnitude = values[:, 0] * values[:, 0] + values[:, 1] * values[:, 1]
    power = lax.dot_general(
        magnitude.reshape(tile_count * orients, width),
        weight[None, :] * ctf * ctf,
        (((1,), (1,)), ((), ())),
        precision=HIGH,
        preferred_element_type=jnp.float32,
    )
    hot = (jnp.arange(NBIN, dtype=jnp.int32)[:, None] == bins[None, :]).astype(jnp.float32)
    offsets = jnp.arange(TSIDE, dtype=jnp.int32) - TSIDE // 2
    cos_t, sin_t = rotation(
        freq_x[None, :],
        freq_y[None, :],
        jnp.repeat(offsets, TSIDE)[:, None],
        jnp.tile(offsets, TSIDE)[:, None],
    )
    group = 2 if tile_count % 2 == 0 else 1
    used = cands * windows * (orients // 2)
    columns = round_up(used + 1, 128)

    def whole(*shape):
        return pl.BlockSpec(shape, lambda i: (0,) * len(shape))

    partial_value = pl.pallas_call(
        functools.partial(score_kernel, orients),
        grid=(tile_count // group,),
        in_specs=[
            pl.BlockSpec((group, pair, orients, width), lambda i: (i, 0, 0, 0)),
            pl.BlockSpec((group * orients, NBIN), lambda i: (i, 0)),
            whole(count, pair * width),
            whole(count, 1),
            whole(NBIN, count),
            whole(windows, count),
            whole(windows, count),
            whole(cands, width),
            whole(cands, width),
        ],
        out_specs=whole(count, columns),
        out_shape=jax.ShapeDtypeStruct((count, columns), jnp.float32),
        scratch_shapes=[
            pltpu.VMEM((group * cands * orients, pair * width), jnp.bfloat16),
            pltpu.VMEM((windows, cands * orients, count), jnp.float32),
            pltpu.VMEM((columns, count), jnp.float32),
        ],
        compiler_params=pltpu.CompilerParams(vmem_limit_bytes=48 * 1024 * 1024),
        name="score",
    )(proj_in, power, weighted, energy, hot, tiles_all, starts_all, cos_t, sin_t)

    blocks = partial_value.reshape(tile_count, local_count, columns)
    blocks = lax.all_to_all(blocks, "tile", split_axis=0, concat_axis=0, tiled=True)
    summed = jnp.sum(blocks, axis=0)
    summed = jnp.sum(lax.all_gather(summed, "shell", axis=0), axis=0)
    scores = summed[:, :used].reshape(local_count, cands, windows * (orients // 2))
    return finish(scores, summed[:, used])


def per_device(particles, projections, noise_weight, tile_list, ori_start, shifts, defocus_bin):
    piece = BOX * lax.axis_size("tile")
    plan = band_plan if particles.shape[2] % piece == 0 else slot_plan
    return plan(
        particles, projections, noise_weight, tile_list, ori_start, shifts, defocus_bin
    )


def solution(mesh):
    in_specs = (
        P("tile", None, "shell"),
        P("tile", None, "shell"),
        P("shell"),
        P("tile", None),
        P("tile", None),
        P("tile", None),
        P("tile"),
    )
    out_specs = (P("tile", None, None), P("tile"))
    return jax.shard_map(
        per_device, mesh=mesh, in_specs=in_specs, out_specs=out_specs, check_vma=False
    )
```
